8 devices in a mesh: dp: 2 (over z, y), sp: 4 (over x, core).
Axes of the slice: x: 2, y: 2, z: 1, core: 2. Of those that a mesh axis runs over, the one named last changes fastest.
Arguments:
- x_in: bfloat16 [4, 1024, 4096], P('dp', 'sp'), parts along dimension 0
- grad_y: bfloat16 [4, 1024, 4096], P('dp', 'sp'), parts along dimension 0
- positions: int32 [4, 1024], P('dp', 'sp'), parts along dimension 0
- g_norm: bfloat16 [4096], replicated
- w_query: bfloat16 [4096, 4096], replicated
- w_key: bfloat16 [4096, 4096], replicated
- w_value: bfloat16 [4096, 4096], replicated
- w_out: bfloat16 [4096, 4096], replicated
- g_query: bfloat16 [4096], replicated
- g_key: bfloat16 [4096], replicated
Outputs:
- output 1: bfloat16 [4, 1024, 4096], P('dp', 'sp'), parts along dimension 0
- output 2: bfloat16 [4, 1024, 4096], P('dp', 'sp'), parts along dimension 0
- output 3: float32 [8192], P(('dp', 'sp')), parts along dimension 0
- output 4: float32 [8192, 4096], P(('dp', 'sp')), parts along dimension 0
- output 5: float32 [8192, 4096], P(('dp', 'sp')), parts along dimension 0
- output 6: float32 [8192, 4096], P(('dp', 'sp')), parts along dimension 0
- output 7: float32 [8192, 4096], P(('dp', 'sp')), parts along dimension 0
- output 8: float32 [8192], P(('dp', 'sp')), parts along dimension 0
- output 9: float32 [8192], P(('dp', 'sp')), parts along dimension 0
There are 2 independent parts. The reference program is written for one: setup_inputs(seed, part) draws one part's arguments, and reference() takes and returns one part's arrays. A program takes and returns all parts, laid end to end along the dimension named above; an argument that names none is the same for every part.
All inputs are finite; a program needn't handle non-finite values.
Results may differ from the reference program's by a relative error of at most 0.0116289.
Values are sent between devices in bfloat16 or wider.
A program may use at most 1 GiB of HBM per device.

```python
import jax
import jax.numpy as jnp
from jax import lax

N_BATCH = 2
SEQ_LEN = 1024
D_MODEL = 4096
N_HEADS = 32
HEAD_DIM = 128
QUERY_BLOCK = min(128, SEQ_LEN)
NORM_EPS = 1e-5
ROPE_BASE = 10000.0
NEG_BIG = -1e30


def setup_inputs(seed: int = 0, part: int = 0) -> dict:
    part_key = jax.random.fold_in(jax.random.key(seed), part)
    key_x, key_dy, key_pos = jax.random.split(part_key, 3)
    weight_keys = jax.random.split(jax.random.key(seed + 1), 9)
    act_shape = (N_BATCH, SEQ_LEN, D_MODEL)
    x_in = jax.random.normal(key_x, act_shape, jnp.float32).astype(jnp.bfloat16)
    grad_y = jax.random.normal(key_dy, act_shape, jnp.float32).astype(jnp.bfloat16)
    tok_idx = jnp.arange(SEQ_LEN, dtype=jnp.int32)
    restart = jax.random.randint(key_pos, (N_BATCH, SEQ_LEN), 0, 256) == 0
    doc_start = lax.cummax(jnp.where(restart, tok_idx[None, :], 0), axis=1)
    positions = (tok_idx[None, :] - doc_start).astype(jnp.int32)
    fan_scale = D_MODEL ** -0.5
    head_q = jnp.repeat(jax.random.uniform(weight_keys[0], (N_HEADS,), jnp.float32, 0.5, 1.5), HEAD_DIM)
    head_k = jnp.repeat(jax.random.uniform(weight_keys[1], (N_HEADS,), jnp.float32, 0.5, 1.5), HEAD_DIM)
    w_shape = (D_MODEL, D_MODEL)
    w_query = (jax.random.normal(weight_keys[2], w_shape, jnp.float32) * fan_scale * head_q[None, :]).astype(jnp.bfloat16)
    w_key = (jax.random.normal(weight_keys[3], w_shape, jnp.float32) * fan_scale * head_k[None, :]).astype(jnp.bfloat16)
    w_value = (jax.random.normal(weight_keys[4], w_shape, jnp.float32) * fan_scale).astype(jnp.bfloat16)
    w_out = (jax.random.normal(weight_keys[5], w_shape, jnp.float32) * fan_scale).astype(jnp.bfloat16)
    g_norm = (1.0 + 0.3 * jax.random.normal(weight_keys[6], (D_MODEL,), jnp.float32)).astype(jnp.bfloat16)
    g_query = (1.7 + 0.4 * jax.random.normal(weight_keys[7], (D_MODEL,), jnp.float32)).astype(jnp.bfloat16)
    g_key = (1.7 + 0.4 * jax.random.normal(weight_keys[8], (D_MODEL,), jnp.float32)).astype(jnp.bfloat16)
    return {'x_in': x_in, 'grad_y': grad_y, 'positions': positions, 'g_norm': g_norm, 'w_query': w_query, 'w_key': w_key, 'w_value': w_value, 'w_out': w_out, 'g_query': g_query, 'g_key': g_key}


def rms_scale(values, gain_vec):
    inv_rms = lax.rsqrt(jnp.mean(values * values, axis=-1, keepdims=True) + NORM_EPS)
    return values * inv_rms * gain_vec


def rope_tables(positions):
    half_dim = HEAD_DIM // 2
    inv_freq = ROPE_BASE ** (-jnp.arange(half_dim, dtype=jnp.float32) * (2.0 / HEAD_DIM))
    angles = positions.astype(jnp.float32)[..., None] * inv_freq
    return jnp.cos(angles)[:, :, None, :], jnp.sin(angles)[:, :, None, :]


def rope_apply(values, cos_t, sin_t):
    half_dim = values.shape[-1] // 2
    first_half = values[..., :half_dim]
    second_half = values[..., half_dim:]
    return jnp.concatenate([first_half * cos_t - second_half * sin_t, second_half * cos_t + first_half * sin_t], axis=-1)


def mat_f32(left_op, right_op):
    return jnp.dot(left_op, right_op, precision=lax.Precision.HIGHEST)


def causal_attention(q_bf, k_bf, v_bf):
    q_f = q_bf.astype(jnp.float32)
    k_f = k_bf.astype(jnp.float32)
    v_f = v_bf.astype(jnp.float32)
    key_pos = jnp.arange(SEQ_LEN)
    qk_scale = HEAD_DIM ** -0.5

    def one_block(q_start):
        q_blk = lax.dynamic_slice_in_dim(q_f, q_start, QUERY_BLOCK, axis=1)
        scores = jnp.einsum('bqhd,bkhd->bhqk', q_blk, k_f, precision=lax.Precision.HIGHEST) * qk_scale
        q_pos = q_start + jnp.arange(QUERY_BLOCK)
        scores = jnp.where(q_pos[:, None] >= key_pos[None, :], scores, NEG_BIG)
        prob_f = jax.nn.softmax(scores, axis=-1)
        return jnp.einsum('bhqk,bkhd->bqhd', prob_f, v_f, precision=lax.Precision.HIGHEST)

    starts = jnp.arange(SEQ_LEN // QUERY_BLOCK) * QUERY_BLOCK
    blocks = lax.map(jax.checkpoint(one_block), starts)
    merged = jnp.moveaxis(blocks, 0, 1).reshape(q_bf.shape)
    return merged.astype(jnp.bfloat16)


def reference(x_in, grad_y, positions, g_norm, w_query, w_key, w_value, w_out, g_query, g_key):
    cos_t, sin_t = rope_tables(positions)
    head_shape = (N_BATCH, SEQ_LEN, N_HEADS, HEAD_DIM)
    flat_shape = (N_BATCH, SEQ_LEN, D_MODEL)

    def forward(x_f, gain_n, wq_f, wk_f, wv_f, wo_f, gain_q, gain_k):
        hidden = rms_scale(x_f, gain_n).astype(jnp.bfloat16).astype(jnp.float32)
        q_raw = mat_f32(hidden, wq_f)
        k_raw = mat_f32(hidden, wk_f)
        v_val = mat_f32(hidden, wv_f).astype(jnp.bfloat16)
        q_rot = rope_apply(rms_scale(q_raw, gain_q).reshape(head_shape), cos_t, sin_t).astype(jnp.bfloat16)
        k_rot = rope_apply(rms_scale(k_raw, gain_k).reshape(head_shape), cos_t, sin_t).astype(jnp.bfloat16)
        attended = causal_attention(q_rot, k_rot, v_val.reshape(head_shape))
        o_proj = mat_f32(attended.reshape(flat_shape).astype(jnp.float32), wo_f)
        return (x_f + o_proj).astype(jnp.bfloat16)

    y_out, pullback = jax.vjp(forward, x_in.astype(jnp.float32), g_norm.astype(jnp.float32), w_query.astype(jnp.float32), w_key.astype(jnp.float32), w_value.astype(jnp.float32), w_out.astype(jnp.float32), g_query.astype(jnp.float32), g_key.astype(jnp.float32))
    cotangents = pullback(grad_y)
    return (y_out, cotangents[0].astype(jnp.bfloat16), cotangents[1], cotangents[2], cotangents[3], cotangents[4], cotangents[5], cotangents[6], cotangents[7])
```

```python
import functools
import math
import jax
import jax.numpy as jnp
from jax import lax
from jax.experimental import pallas as pl
from jax.experimental.pallas import tpu as pltpu
from jax.sharding import PartitionSpec as P

HEAD_DIM = 128
NORM_EPS = 1e-5
ROPE_BASE = 10000.0
NEG_BIG = -1e30
PIECE = 256
PIECES = range(4)
PAIR = range(2)
TILE = 512
HEADS_STEP = 2
VMEM_LIMIT = 60 * 1024 * 1024

SIBLING = [(0, 1), (1, 0), (2, 3), (3, 2)]
CROSS = [(0, 2), (2, 0), (1, 3), (3, 1)]
NT = (((1,), (1,)), ((), ()))
NN = (((1,), (0,)), ((), ()))


def dot(left, right, dims=NN):
    return lax.dot_general(left, right, dims, preferred_element_type=jnp.float32)


def params(sem=1):
    return pltpu.CompilerParams(dimension_semantics=("arbitrary",) * sem, vmem_limit_bytes=VMEM_LIMIT)


def cost(flops, nbytes, trans=0):
    return pl.CostEstimate(flops=int(flops), bytes_accessed=int(nbytes), transcendentals=int(trans))


def core_tile(tile, core, per=2):
    return (tile // per * 2 + core) * per + tile % per


def half_block(i, core):
    return i % 2 * 2 + jnp.bitwise_xor(core, i // 2)


def once(shape, index_map):
    return pl.BlockSpec(shape, index_map, pipeline_mode=pl.Buffered(1))


def fixed(shape, **mode):
    return pl.BlockSpec(shape, lambda j, m: (0,) * len(shape), **mode)


def whole(shape):
    return fixed(shape, pipeline_mode=pl.Buffered(1))


def columns(shape):
    return pl.BlockSpec(shape, lambda j, m: (0,) * (len(shape) - 1) + (j,))


def scalar_grid(steps, in_specs, out_specs, scratch=()):
    shape = (steps,)
    return pltpu.PrefetchScalarGridSpec(num_scalar_prefetch=1, grid=shape, in_specs=in_specs, out_specs=out_specs, scratch_shapes=scratch)


def col_sum(val):
    return val.sum(axis=0, keepdims=True)


def row_sum(val):
    return val.sum(axis=-1, keepdims=True)


def spread(val):
    return jnp.broadcast_to(val, (PIECE, HEAD_DIM))


def turn(val):
    return pltpu.roll(val, HEAD_DIM // 2, 1)


def qkv_project(meta, first, second, w_query, w_key, w_value):
    d_model = w_query.shape[0]
    half = d_model // 2
    n_tiles = half // TILE
    n_seq = first.shape[0]
    span = n_seq * PIECE

    def body(meta_ref, a_ref, b_ref, wq_ref, wk_ref, wv_ref, q_ref, k_ref, v_ref, sq_ref, lhs):
        step = pl.program_id(0)

        @pl.when(step == 0)
        def _():
            lhs[0:span, :] = a_ref[...].reshape(span, d_model)
            lhs[span:, :] = b_ref[...].reshape(span, d_model)
            sq_ref[...] = jnp.zeros_like(sq_ref)

        def put(out_ref, acc):
            for piece in PAIR:
                out_ref[:, piece] = acc[piece * span:(piece + 1) * span].reshape(n_seq, PIECE, acc.shape[-1])

        def normed_out(w_ref, out_ref, which):
            acc = dot(lhs[...], w_ref[...])
            put(out_ref, acc)
            square = acc * acc
            part = square[:, 0:128]
            for lane in range(128, TILE, 128):
                part = part + square[:, lane:lane + 128]
            for piece in PAIR:
                sq_ref[which, :, piece] += part[piece * span:(piece + 1) * span].reshape(n_seq, PIECE, 128)

        @pl.when(step < n_tiles)
        def _():
            normed_out(wq_ref, q_ref, 0)

        @pl.when((step >= n_tiles) & (step < 2 * n_tiles))
        def _():
            normed_out(wk_ref, k_ref, 1)

        @pl.when(step >= 2 * n_tiles)
        def _():
            put(v_ref, dot(lhs[...], wv_ref[...]).astype(jnp.bfloat16))

    def phase(step, which):
        return jnp.clip(step - which * n_tiles, 0, n_tiles - 1)

    def w_spec(which):
        return pl.BlockSpec((d_model, TILE), lambda j, m: (0, core_tile(phase(j, which), m[1])))

    def o_spec(which):
        return pl.BlockSpec((n_seq, 2, PIECE, TILE), lambda j, m: (0, 0, 0, phase(j, which)))

    act = whole((n_seq, PIECE, d_model))
    sums = (2, n_seq, 2, PIECE, 128)
    grid_spec = scalar_grid(
        3 * n_tiles, in_specs=[act, act, w_spec(0), w_spec(1), w_spec(2)],
        out_specs=[o_spec(0), o_spec(1), o_spec(2), fixed(sums)],
        scratch=[pltpu.VMEM((2 * span, d_model), jnp.bfloat16)])
    shape = (n_seq, 2, PIECE, half)
    return pl.pallas_call(
        body, grid_spec=grid_spec, name="qkv",
        out_shape=[jax.ShapeDtypeStruct(shape, jnp.float32), jax.ShapeDtypeStruct(shape, jnp.float32),
                   jax.ShapeDtypeStruct(shape, jnp.bfloat16), jax.ShapeDtypeStruct(sums, jnp.float32)],
        compiler_params=params(), cost_estimate=cost(2 * 2 * span * d_model * 3 * half, 3 * d_model * half * 2 + 2 ** 24),
    )(meta, first, second, w_query, w_key, w_value)


def attn_grad(meta, first, second, w_out):
    d_model = w_out.shape[0]
    half = d_model // 2
    n_seq = first.shape[0]
    span = n_seq * PIECE

    def body(meta_ref, a_ref, b_ref, w_ref, o_ref, lhs):
        @pl.when(pl.program_id(0) == 0)
        def _():
            lhs[0:span, :] = a_ref[...].reshape(span, d_model)
            lhs[span:, :] = b_ref[...].reshape(span, d_model)

        acc = dot(lhs[...], w_ref[...], NT).astype(jnp.bfloat16)
        for piece in PAIR:
            o_ref[:, piece] = acc[piece * span:(piece + 1) * span].reshape(n_seq, PIECE, TILE)

    act = whole((n_seq, PIECE, d_model))
    grid_spec = scalar_grid(
        half // TILE, in_specs=[act, act, pl.BlockSpec((TILE, d_model), lambda j, m: (core_tile(j, m[1]), 0))],
        out_specs=columns((n_seq, 2, PIECE, TILE)),
        scratch=[pltpu.VMEM((2 * span, d_model), jnp.bfloat16)])
    return pl.pallas_call(
        body, grid_spec=grid_spec, name="attn_grad",
        out_shape=jax.ShapeDtypeStruct((n_seq, 2, PIECE, half), jnp.bfloat16),
        compiler_params=params(), cost_estimate=cost(2 * 2 * span * d_model * half, d_model * half * 2 + 2 ** 23),
    )(meta, first, second, w_out)


def attention(meta, q_own, q_far, k_own, k_far, v_own, v_far, do_own, do_far, sums, cos_t, sin_t, g_query, g_key, seq, carried):
    half = q_own.shape[-1]
    n_heads = half // HEAD_DIM
    seq_len = 4 * PIECE
    wide = HEADS_STEP * HEAD_DIM
    scale = HEAD_DIM ** -0.5
    exp_scale = scale * math.log2(math.e)
    n_carried = len(carried)

    def body(meta_ref, qo, qx, ko, kx, vo, vx, doo, dox, no, ns, fo, fs, cos_ref, sin_ref, gq_ref, gk_ref, *rest):
        rest = rest[n_carried:]
        a_ref, dq_ref, dk_ref, dv_ref, at_ref, stat_ref, inv_ref, gain_ref, qs, ks, vs, dos, v_t, k_t, do_t, q_t, outs, dqs, dks, dvs = rest
        device, core = meta_ref[0], meta_ref[1]

        @pl.when(pl.program_id(0) == 0)
        def _():
            stat_ref[...] = jnp.zeros_like(stat_ref)
            for which in PAIR:
                for r in PIECES:
                    own, other = ((no, ns), (fo, fs))[r // 2]
                    both = own[which, 0, r % 2] + other[which, 0, 1 - r % 2]
                    inv = lax.rsqrt(row_sum(both) / (2 * half) + NORM_EPS)
                    inv_ref[which, r] = spread(inv)

        gains = (gq_ref[...].astype(jnp.float32), gk_ref[...].astype(jnp.float32))
        heads = [slice(i * HEAD_DIM, (i + 1) * HEAD_DIM) for i in range(HEADS_STEP)]

        def place(r):
            return pl.ds(pl.multiple_of(jnp.bitwise_xor(device, r) * PIECE, PIECE), PIECE)

        def normed(r, which, lanes):
            src = ((qo, qx), (ko, kx))[which][r // 2]
            return src[0, r % 2, :, lanes] * inv_ref[which, r]

        for r in PIECES:
            rows = place(r)
            vs[rows, :] = (vo, vx)[r // 2][0, r % 2]
            dos[rows, :] = (doo, dox)[r // 2][0, r % 2]
            for lanes in heads:
                for which, dst in ((0, qs), (1, ks)):
                    val = normed(r, which, lanes) * gains[which][:, lanes]
                    rot = val * cos_ref[r] + turn(val) * sin_ref[r]
                    dst[rows, lanes] = rot.astype(jnp.bfloat16)
        for lanes in heads:
            v_t[lanes, :] = vs[:, lanes].T
            k_t[lanes, :] = ks[:, lanes].T
            do_t[lanes, :] = dos[:, lanes].T
            q_t[lanes, :] = qs[:, lanes].T

        key_idx = lax.broadcasted_iota(jnp.int32, (PIECE, PIECE), 0)
        query_idx = lax.broadcasted_iota(jnp.int32, (PIECE, PIECE), 1)
        allowed = key_idx <= query_idx

        def products(unit):
            lanes, qi = unit
            cols = slice(qi * PIECE, (qi + 1) * PIECE)
            keys = (qi + 1) * PIECE
            return dot(ks[0:keys, lanes], q_t[lanes, cols]), dot(vs[0:keys, lanes], do_t[lanes, cols])

        order = [(lanes, qi) for qi in (3, 2, 1, 0) for lanes in heads]
        ahead = products(order[0])
        for pos, (lanes, qi) in enumerate(order):
            scores, d_probs = ahead
            if pos + 1 < len(order):
                ahead = products(order[pos + 1])
            low = qi * PIECE
            high = low + PIECE
            diag = jnp.where(allowed, scores[low:high, :], NEG_BIG)
            parts = [scores[0:low, :], diag] if qi else [diag]
            d_parts = [d_probs[0:low, :], d_probs[low:high, :]] if qi else [d_probs]
            top = parts[0].max(axis=0, keepdims=True)
            for s in parts[1:]:
                top = jnp.maximum(top, s.max(axis=0, keepdims=True))
            probs = [jnp.exp2((s - top) * exp_scale) for s in parts]
            total = sum(col_sum(p) for p in probs)
            inv_total = 1.0 / total
            probs = [p * inv_total for p in probs]
            row_dot = sum(col_sum((p * d)) for p, d in zip(probs, d_parts))
            d_scores = [(p * (d - row_dot)).astype(jnp.bfloat16) for p, d in zip(probs, d_parts)]
            probs_bf = [p.astype(jnp.bfloat16) for p in probs]
            d_scores = jnp.concatenate(d_scores, axis=0) if qi else d_scores[0]
            probs_bf = jnp.concatenate(probs_bf, axis=0) if qi else probs_bf[0]
            out_t = dot(v_t[lanes, 0:high], probs_bf)
            dq_t = dot(k_t[lanes, 0:high], d_scores)
            outs[low:high, lanes] = out_t.T.astype(jnp.bfloat16)
            spot = jnp.bitwise_xor(jnp.bitwise_xor(device, core), qi)
            at_ref[lanes, pl.ds(pl.multiple_of(spot * PIECE, PIECE), PIECE)] = out_t.astype(jnp.bfloat16)
            dqs[low:high, lanes] = dq_t.T
            dv_term = dot(probs_bf, dos[low:high, lanes])
            dk_term = dot(d_scores, qs[low:high, lanes])
            if qi == 3:
                dvs[:, lanes] = dv_term
                dks[:, lanes] = dk_term
            else:
                dvs[0:high, lanes] += dv_term
                dks[0:high, lanes] += dk_term

        gain_sums = [[0.0] * HEADS_STEP, [0.0] * HEADS_STEP]
        for r in PIECES:
            rows = place(r)
            slot = jnp.bitwise_xor(core, r)
            a_ref[0, slot] = outs[rows, :]
            dv_ref[0, slot] = dvs[rows, :].astype(jnp.bfloat16)
            for i, lanes in enumerate(heads):
                for which, src, dst in ((0, dqs, dq_ref), (1, dks, dk_ref)):
                    grad_bf = (src[rows, lanes] * scale).astype(jnp.bfloat16)
                    dst[0, slot, :, lanes] = grad_bf
                    grad = grad_bf.astype(jnp.float32)
                    back = grad * cos_ref[r] - turn(grad) * sin_ref[r]
                    term = back * normed(r, which, lanes)
                    gain_sums[which][i] = gain_sums[which][i] + col_sum(term)
                    stat_ref[which, r] += term * gains[which][:, lanes]
        for i, lanes in enumerate(heads):
            gain_ref[0, 0, :, lanes] = gain_sums[0][i]
            gain_ref[0, 1, :, lanes] = gain_sums[1][i]

    per_block = 8 // HEADS_STEP

    def act(arr):
        pick = seq if arr.shape[0] > 1 else 0
        return pl.BlockSpec((1, 2, PIECE, wide), lambda j, m: (pick, 0, 0, j))

    acts = [q_own, q_far, k_own, k_far, v_own, v_far, do_own, do_far]
    lane_sums = once((2, 1, 2, PIECE, HEAD_DIM), lambda j, m: (0, seq, 0, 0, 0))
    table = whole((4, PIECE, HEAD_DIM))
    gain = pl.BlockSpec((1, wide), lambda j, m: (0, core_tile(j, m[1], per_block)))
    big = pl.BlockSpec((1, 4, PIECE, wide), lambda j, m: (seq, 0, 0, j))
    col_bf = pltpu.VMEM((seq_len, wide), jnp.bfloat16)
    row_bf = pltpu.VMEM((wide, seq_len), jnp.bfloat16)
    col_f = pltpu.VMEM((seq_len, wide), jnp.float32)
    n_steps = n_heads // HEADS_STEP
    stat_spec = fixed((2, 4, PIECE, HEAD_DIM))
    stat_shape = jax.ShapeDtypeStruct((2, 4, PIECE, HEAD_DIM), jnp.float32)
    grid_spec = scalar_grid(
        n_steps, in_specs=[act(arr) for arr in acts] + [lane_sums] * 4 + [table, table, gain, gain] + [pl.BlockSpec(memory_space=pl.ANY)] * n_carried,
        out_specs=[big] * 4 + [pl.BlockSpec((wide, seq_len), lambda j, m: (j, seq)),
                               stat_spec, stat_spec,
                               pl.BlockSpec((1, 2, 1, wide), lambda j, m: (j, 0, 0, 0))],
        scratch=[col_bf] * 4 + [row_bf] * 4 + [col_bf] + [col_f] * 3)
    full = jax.ShapeDtypeStruct((2, 4, PIECE, half), jnp.bfloat16)
    flops = 6 * 2 * HEAD_DIM * 10 * PIECE * PIECE * n_heads
    return pl.pallas_call(
        body, grid_spec=grid_spec, name="attention",
        out_shape=[full] * 4 + [jax.ShapeDtypeStruct((half, 2 * seq_len), jnp.bfloat16), stat_shape, stat_shape,
                                jax.ShapeDtypeStruct((n_steps, 2, 1, wide), jnp.float32)],
        input_output_aliases={17 + i: i for i in range(n_carried)},
        compiler_params=params(), cost_estimate=cost(2 * flops, 5 * 2 ** 23, 10 * PIECE * PIECE * n_heads),
    )(meta, *acts, *sums, cos_t, sin_t, g_query, g_key, *carried)


def finish_grads(meta, d_query, d_key, raws, stats, stats_sib, invs, cos_t, sin_t, g_query, g_key):
    half = d_query.shape[-1]
    wide = 256
    n_steps = half // wide

    def body(meta_ref, dq_ref, dk_ref, qn, qf, kn, kf, s0, s1, t0, t1, i0, i1, cos_ref, sin_ref, gq_ref, gk_ref, oq_ref, ok_ref, mean):
        core = meta_ref[1]

        @pl.when(pl.program_id(0) == 0)
        def _():
            for seq in PAIR:
                for which in PAIR:
                    for r in PIECES:
                        both = (s0, s1)[seq][which, r] + (t0, t1)[seq][which, r ^ 1]
                        row = row_sum(both) / (2 * half)
                        mean[seq, which, r] = spread(row)

        for which, (d_ref, near, far, g_ref, o_ref) in enumerate(((dq_ref, qn, qf, gq_ref, oq_ref), (dk_ref, kn, kf, gk_ref, ok_ref))):
            for seq in PAIR:
                for r in PIECES:
                    slot = jnp.bitwise_xor(core, r)
                    scl = (i0, i1)[seq][which, r]
                    for lane in range(0, wide, HEAD_DIM):
                        lanes = slice(lane, lane + HEAD_DIM)
                        grad = d_ref[seq, slot, :, lanes].astype(jnp.float32)
                        back = grad * cos_ref[seq, r] - turn(grad) * sin_ref[seq, r]
                        normed = (near, far)[r // 2][seq, r % 2, :, lanes] * scl
                        gain = g_ref[:, lanes].astype(jnp.float32)
                        o_ref[seq, slot, :, lanes] = (scl * (back * gain - normed * mean[seq, which, r])).astype(jnp.bfloat16)


    big = columns((2, 4, PIECE, wide))
    raw = columns((2, 2, PIECE, wide))
    table = whole((2, 4, PIECE, HEAD_DIM))
    gain = pl.BlockSpec((1, wide), lambda j, m: (0, core_tile(j, m[1], 4)))
    grid_spec = scalar_grid(
        n_steps, in_specs=[big, big] + [raw] * 4 + [table] * 8 + [gain, gain],
        out_specs=[big, big], scratch=[pltpu.VMEM((2, 2, 4, PIECE, HEAD_DIM), jnp.float32)])
    return pl.pallas_call(
        body, grid_spec=grid_spec, name="finish",
        out_shape=[jax.ShapeDtypeStruct(d_query.shape, jnp.bfloat16)] * 2,
        compiler_params=params(), cost_estimate=cost(20 * d_query.size, 16 * d_query.size),
    )(meta, d_query, d_key, *raws, *stats, *stats_sib, *invs, cos_t, sin_t, g_query, g_key)


def rows_transposed(meta, own, sib, far, far_sib):
    d_model = own.shape[-1]
    rows = d_model // 4

    def body(meta_ref, *refs):
        core = meta_ref[1]
        for seq in PAIR:
            for r in PIECES:
                spot = pl.multiple_of((seq * 4 + jnp.bitwise_xor(core, r)) * PIECE, PIECE)
                refs[4][:, pl.ds(spot, PIECE)] = refs[r][seq].T

    act = pl.BlockSpec((2, PIECE, rows), lambda j, m: (0, 0, m[0]))
    grid_spec = scalar_grid(
        1, in_specs=[act] * 4,
        out_specs=fixed((rows, 8 * PIECE)))
    return pl.pallas_call(
        body, grid_spec=grid_spec, name="rows_transposed",
        out_shape=jax.ShapeDtypeStruct((rows, 8 * PIECE), jnp.bfloat16),
        compiler_params=params(), cost_estimate=cost(8 * PIECE * rows, 4 * 8 * PIECE * rows),
    )(meta, own, sib, far, far_sib)


def out_project(meta, a_own, a_sib, w_out, x_loc):
    d_model = w_out.shape[0]
    half = d_model // 2
    quarter = half // 2

    def body(meta_ref, own_ref, sib_ref, w0, w1, w2, w3, x_ref, y_ref, lhs):
        @pl.when(pl.program_id(0) == 0)
        def _():
            for seq in PAIR:
                lhs[seq * PIECE:(seq + 1) * PIECE, 0:half] = own_ref[seq, 0]
                lhs[seq * PIECE:(seq + 1) * PIECE, half:] = sib_ref[seq]

        acc = dot(lhs[:, 0:quarter], w0[...])
        for i, w in enumerate((w1, w2, w3), 1):
            acc = acc + dot(lhs[:, i * quarter:(i + 1) * quarter], w[...])
        y_ref[...] = (x_ref[...].astype(jnp.float32) + acc.reshape(x_ref.shape)).astype(jnp.bfloat16)

    def w_spec(i):
        return pl.BlockSpec((quarter, TILE), lambda j, m: (half_block(i, m[1]), j))

    act = columns((2, PIECE, TILE))
    grid_spec = scalar_grid(
        d_model // TILE, in_specs=[once((2, 1, PIECE, half), lambda j, m: (0, m[1], 0, 0)), whole((2, PIECE, half))]
        + [w_spec(i) for i in range(4)] + [act],
        out_specs=act, scratch=[pltpu.VMEM((2 * PIECE, d_model), jnp.bfloat16)])
    return pl.pallas_call(
        body, grid_spec=grid_spec, name="out_project",
        out_shape=jax.ShapeDtypeStruct(x_loc.shape, jnp.bfloat16),
        compiler_params=params(), cost_estimate=cost(2 * 2 * PIECE * d_model * d_model, d_model * d_model * 2 + 2 ** 24),
    )(meta, a_own, a_sib, w_out, w_out, w_out, w_out, x_loc)


def hidden_grad(meta, owns, sibs, weights):
    d_model = weights[0].shape[0]
    half = d_model // 2
    quarter = half // 2

    def body(meta_ref, *refs):
        acts, ws, o_ref = refs[:6], refs[6:18], refs[18]
        acc = None
        for i in range(3):
            for part in PAIR:
                lhs = acts[2 * i + part][...].reshape(2 * PIECE, half)
                for blk in PAIR:
                    term = dot(lhs[:, blk * quarter:(blk + 1) * quarter], ws[4 * i + 2 * part + blk][...], NT)
                    acc = term if acc is None else acc + term
        o_ref[...] = acc.reshape(o_ref.shape)

    def w_spec(i):
        return pl.BlockSpec((TILE, quarter), lambda j, m: (j, half_block(i, m[1])))

    own = once((2, 1, PIECE, half), lambda j, m: (0, m[1], 0, 0))
    grid_spec = scalar_grid(
        d_model // TILE, in_specs=[own] * 6 + [w_spec(i) for i in range(4)] * 3,
        out_specs=columns((2, PIECE, TILE)))
    acts = [a for pair in zip(owns, sibs) for a in pair]
    mats = [w for w in weights for _ in range(4)]
    return pl.pallas_call(
        body, grid_spec=grid_spec, name="hidden_grad",
        out_shape=jax.ShapeDtypeStruct((2, PIECE, d_model), jnp.float32),
        compiler_params=params(), cost_estimate=cost(6 * 2 * PIECE * d_model * d_model, 6 * d_model * d_model + 2 ** 24),
    )(meta, *acts, *mats)


def weight_grads(meta, rows_t, owns, sibs):
    rows, tokens = rows_t.shape
    half = owns[0].shape[-1]
    n_tiles = half // TILE
    per = 2 * n_tiles
    n_mats = len(owns)

    def body(meta_ref, lhs_ref, *refs):
        step = pl.program_id(0)
        for i in range(2 * n_mats):
            @pl.when((step >= i * n_tiles) & (step < (i + 1) * n_tiles))
            def _(i=i):
                refs[2 * n_mats + i // 2][...] = dot(lhs_ref[...], refs[i][...])

    def in_spec(i):
        return pl.BlockSpec((tokens, TILE), lambda j, m: (0, jnp.clip(j - i * n_tiles, 0, n_tiles - 1)))

    def out_spec(i):
        def tile(j, m):
            t = jnp.clip(j - i * per, 0, per - 1)
            return 0, core_tile(t % n_tiles, jnp.bitwise_xor(m[1], t // n_tiles))
        return pl.BlockSpec((rows, TILE), tile)

    grid_spec = scalar_grid(
        per * n_mats, in_specs=[whole((rows, tokens))] + [in_spec(i) for i in range(2 * n_mats)],
        out_specs=[out_spec(i) for i in range(n_mats)])
    mats = [a.reshape(tokens, half) for pair in zip(owns, sibs) for a in pair]
    return pl.pallas_call(
        body, grid_spec=grid_spec, name="weight_grads",
        out_shape=[jax.ShapeDtypeStruct((rows, 2 * half), jnp.float32)] * n_mats,
        compiler_params=params(),
        cost_estimate=cost(n_mats * 2 * rows * tokens * 2 * half, n_mats * (rows * half * 8 + tokens * half * 4)),
    )(meta, rows_t, *mats)


def out_weight_grad(meta, a_t, pieces):
    tokens = a_t.shape[1]
    rows = a_t.shape[0] // 2
    d_model = pieces[0][0].shape[-1]

    def body(meta_ref, a_ref, *refs):
        core = meta_ref[1]
        acc = None
        for i in range(8):
            spot = pl.multiple_of((i // 4 * 4 + jnp.bitwise_xor(core, i % 4)) * PIECE, PIECE)
            term = dot(a_ref[:, pl.ds(spot, PIECE)], refs[i][0])
            acc = term if acc is None else acc + term
        refs[8][...] = acc

    def spec(seq):
        return pl.BlockSpec((1, PIECE, TILE), lambda j, m: (seq, 0, j))

    grid_spec = scalar_grid(
        d_model // TILE, in_specs=[once((rows, tokens), lambda j, m: (m[2], 0))] + [spec(seq) for _, seq in pieces],
        out_specs=columns((rows, TILE)))
    return pl.pallas_call(
        body, grid_spec=grid_spec, name="out_weight_grad",
        out_shape=jax.ShapeDtypeStruct((rows, d_model), jnp.float32),
        compiler_params=params(), cost_estimate=cost(2 * rows * tokens * d_model, rows * d_model * 4 + tokens * d_model * 2),
    )(meta, a_t, *[arr for arr, _ in pieces])


def after(value, *others):
    return lax.optimization_barrier((value,) + others)[0]


def solution(mesh):
    to_sibling = functools.partial(lax.ppermute, axis_name='sp', perm=SIBLING)
    to_far = functools.partial(lax.ppermute, axis_name='sp', perm=CROSS)

    def device_step(x_loc, grad_y, positions, g_norm, w_query, w_key, w_value, w_out, g_query, g_key):
        n_batch, loc_len, d_model = x_loc.shape
        device = lax.axis_index('sp')
        core = device % 2
        chip = device // 2
        meta = jnp.stack([device, core, chip]).astype(jnp.int32)
        gq = g_query.reshape(1, d_model)
        gk = g_key.reshape(1, d_model)

        pos_far = to_far(positions)
        pos_sib = to_sibling(positions)
        x_f = x_loc.astype(jnp.float32)
        x_inv = lax.rsqrt(jnp.mean(x_f * x_f, axis=-1, keepdims=True) + NORM_EPS)
        hidden = (x_f * x_inv * g_norm.astype(jnp.float32)).astype(jnp.bfloat16)
        hidden, gy, pos_far = lax.optimization_barrier((hidden, grad_y, pos_far))

        h_sib = to_sibling(hidden)
        h_far = to_far(hidden)
        gy_sib = to_sibling(gy)
        gy_late = after(gy, h_sib)
        gy_far = [to_far(gy_late[0:1]), to_far(gy_late[1:2])]

        qn, kn, vn, sums_near = qkv_project(meta, hidden, h_sib, w_query, w_key, w_value)
        sums_near_sib = to_sibling(sums_near)
        pos_fs = to_sibling(after(pos_far, sums_near))
        d_near = attn_grad(meta, gy, after(gy_sib, sums_near), w_out)
        h_far = after(h_far, d_near)
        h_fs = to_sibling(h_far)

        pos_all = jnp.stack([positions, pos_sib, pos_far, pos_fs], axis=1)
        half_dim = HEAD_DIM // 2
        inv_freq = ROPE_BASE ** (-jnp.arange(half_dim, dtype=jnp.float32) * (2.0 / HEAD_DIM))
        angles = pos_all.astype(jnp.float32)[..., None] * inv_freq
        cos_h, sin_h = jnp.cos(angles), jnp.sin(angles)
        cos_t = jnp.concatenate([cos_h, cos_h], axis=-1)
        sin_t = jnp.concatenate([-sin_h, sin_h], axis=-1)

        qf, kf, vf, sums_far = qkv_project(meta, h_far, h_fs, w_query, w_key, w_value)
        sums_far_sib = to_sibling(sums_far)
        sums = (sums_near, sums_near_sib, sums_far, sums_far_sib)
        gy_far[0] = after(gy_far[0], sums_far)
        gy_fs = [to_sibling(gy_far[0])]
        rows_t = rows_transposed(meta, hidden, h_sib, after(h_far, sums_far), h_fs)
        d_far = [attn_grad(meta, gy_far[0], after(gy_fs[0], rows_t), w_out)]

        stats, invs, gains = [], [], 0.0
        carried = ()
        for seq in PAIR:
            if seq == 1:
                gy_far[1] = after(gy_far[1], stats[0])
                gy_fs.append(to_sibling(gy_far[1]))
                d_far.append(attn_grad(meta, gy_far[1], gy_fs[1], w_out))
            *carried, stat, inv, gain = attention(meta, qn, qf, kn, kf, vn, vf, d_near, d_far[seq], sums, cos_t[seq], sin_t[seq], gq, gk, seq, carried)
            stats.append(stat)
            invs.append(inv)
            gains = gains + gain
        attended, dq_rot, dk_rot, dv, a_t = carried
        stats_sib = [to_sibling(stat) for stat in stats]
        a_out = lax.dynamic_index_in_dim(attended, 1 - core, axis=1, keepdims=False)
        a_sib = to_sibling(after(a_out, *stats_sib))
        dv_sib = to_sibling(after(dv, *stats_sib))
        dq, dk = finish_grads(meta, dq_rot, dk_rot, (qn, qf, kn, kf), stats, stats_sib, invs, cos_t, sin_t, gq, gk)
        dq, dk, a_sib, dv_sib = lax.optimization_barrier((dq, dk, a_sib, dv_sib))
        dq_sib, dk_sib = to_sibling(dq), to_sibling(dk)

        gy_pieces = []
        for seq in PAIR:
            gy_pieces += [(gy, seq), (gy_sib, seq), (gy_far[seq], 0), (gy_fs[seq], 0)]
        grad_w_out = out_weight_grad(meta, after(a_t, dq), gy_pieces)
        a_sib, grad_w_out = lax.optimization_barrier((a_sib, grad_w_out))
        y_out = out_project(meta, attended, a_sib, w_out, x_loc)
        dq_sib, dk_sib, y_out = lax.optimization_barrier((dq_sib, dk_sib, y_out))

        d_hidden = hidden_grad(meta, [dq, dk, dv], [dq_sib, dk_sib, dv_sib], [w_query, w_key, w_value])
        x_hat = x_f * x_inv
        d_normed = d_hidden * g_norm.astype(jnp.float32)
        d_x = x_inv * (d_normed - x_hat * jnp.mean(d_normed * x_hat, axis=-1, keepdims=True))
        grad_x = (grad_y.astype(jnp.float32) + d_x).astype(jnp.bfloat16)
        part = jnp.sum(d_hidden * x_hat, axis=(0, 1)).reshape(2, 2, d_model // 4)
        part = lax.dynamic_index_in_dim(part, chip, 0, False) + to_far(lax.dynamic_index_in_dim(part, 1 - chip, 0, False))
        grad_g_norm = lax.dynamic_index_in_dim(part, core, 0, False) + to_sibling(lax.dynamic_index_in_dim(part, 1 - core, 0, False))

        grad_w_value, grad_w_query, grad_w_key = weight_grads(meta, after(rows_t, grad_x), [dv, dq, dk], [dv_sib, dq_sib, dk_sib])
        gains = gains.reshape(2, -1, 2, HEADS_STEP * HEAD_DIM)
        gains = lax.dynamic_index_in_dim(gains, chip, 0, False)
        grad_g_query = gains[:, 0].reshape(-1)
        grad_g_key = gains[:, 1].reshape(-1)
        return y_out, grad_x, grad_g_norm, grad_w_query, grad_w_key, grad_w_value, grad_w_out, grad_g_query, grad_g_key

    seq_spec = P('dp', 'sp', None)
    mat_rep = P(None, None)
    vec_rep = P(None)
    row_spec = P(('dp', 'sp'), None)
    vec_spec = P(('dp', 'sp'))
    return jax.shard_map(device_step, mesh=mesh, in_specs=(seq_spec, seq_spec, P('dp', 'sp'), vec_rep, mat_rep, mat_rep, mat_rep, mat_rep, vec_rep, vec_rep), out_specs=(seq_spec, seq_spec, vec_spec, row_spec, row_spec, row_spec, row_spec, vec_spec, vec_spec), check_vma=False)
```

```python
import functools
import math
import jax
import jax.numpy as jnp
from jax import lax
from jax.experimental import pallas as pl
from jax.experimental.pallas import tpu as pltpu
from jax.sharding import PartitionSpec as P

HEAD_DIM = 128
NORM_EPS = 1e-5
ROPE_BASE = 10000.0
NEG_BIG = -1e30
PIECE = 256
PIECES = range(4)
PAIR = range(2)
TILE = 512
HEADS_STEP = 2
VMEM_LIMIT = 60 * 1024 * 1024

SIBLING = [(0, 1), (1, 0), (2, 3), (3, 2)]
CROSS = [(0, 2), (2, 0), (1, 3), (3, 1)]
NT = (((1,), (1,)), ((), ()))
NN = (((1,), (0,)), ((), ()))


def dot(left, right, dims=NN):
    return lax.dot_general(left, right, dims, preferred_element_type=jnp.float32)


def params(sem=1):
    return pltpu.CompilerParams(dimension_semantics=("arbitrary",) * sem, vmem_limit_bytes=VMEM_LIMIT)


def cost(flops, nbytes, trans=0):
    return pl.CostEstimate(flops=int(flops), bytes_accessed=int(nbytes), transcendentals=int(trans))


def core_tile(tile, core, per=2):
    return (tile // per * 2 + core) * per + tile % per


def half_block(i, core):
    return i % 2 * 2 + jnp.bitwise_xor(core, i // 2)


def once(shape, index_map):
    return pl.BlockSpec(shape, index_map, pipeline_mode=pl.Buffered(1))


def fixed(shape, **mode):
    return pl.BlockSpec(shape, lambda j, m: (0,) * len(shape), **mode)


def whole(shape):
    return fixed(shape, pipeline_mode=pl.Buffered(1))


def columns(shape):
    return pl.BlockSpec(shape, lambda j, m: (0,) * (len(shape) - 1) + (j,))


def scalar_grid(steps, in_specs, out_specs, scratch=()):
    shape = (steps,)
    return pltpu.PrefetchScalarGridSpec(num_scalar_prefetch=1, grid=shape, in_specs=in_specs, out_specs=out_specs, scratch_shapes=scratch)


def col_sum(val):
    return val.sum(axis=0, keepdims=True)


def row_sum(val):
    return val.sum(axis=-1, keepdims=True)


def spread(val):
    return jnp.broadcast_to(val, (PIECE, HEAD_DIM))


def turn(val):
    return pltpu.roll(val, HEAD_DIM // 2, 1)


def input_norm(x_loc, g_norm):
    d_model = x_loc.shape[-1]
    rows = 128

    def body(x_ref, g_ref, o_ref):
        val = x_ref[0].astype(jnp.float32)
        inv = lax.rsqrt(row_sum(val * val) / d_model + NORM_EPS)
        o_ref[0] = (val * inv * g_ref[...].astype(jnp.float32)).astype(jnp.bfloat16)

    act = pl.BlockSpec((1, rows, d_model), lambda b, i: (b, i, 0))
    return pl.pallas_call(
        body, grid=(x_loc.shape[0], x_loc.shape[1] // rows), name="input_norm",
        in_specs=[act, pl.BlockSpec((1, d_model), lambda b, i: (0, 0))], out_specs=act,
        out_shape=jax.ShapeDtypeStruct(x_loc.shape, jnp.bfloat16), compiler_params=params(2),
        cost_estimate=cost(8 * x_loc.size, 4 * x_loc.size))(x_loc, g_norm)


def qkv_project(meta, first, second, w_query, w_key, w_value):
    d_model = w_query.shape[0]
    half = d_model // 2
    n_tiles = half // TILE
    n_seq = first.shape[0]
    span = n_seq * PIECE

    def body(meta_ref, a_ref, b_ref, wq_ref, wk_ref, wv_ref, q_ref, k_ref, v_ref, sq_ref, lhs):
        step = pl.program_id(0)

        @pl.when(step == 0)
        def _():
            lhs[0:span, :] = a_ref[...].reshape(span, d_model)
            lhs[span:, :] = b_ref[...].reshape(span, d_model)
            sq_ref[...] = jnp.zeros_like(sq_ref)

        def put(out_ref, acc):
            for piece in PAIR:
                out_ref[:, piece] = acc[piece * span:(piece + 1) * span].reshape(n_seq, PIECE, acc.shape[-1])

        def normed_out(w_ref, out_ref, which):
            acc = dot(lhs[...], w_ref[...])
            put(out_ref, acc)
            square = acc * acc
            part = square[:, 0:128]
            for lane in range(128, TILE, 128):
                part = part + square[:, lane:lane + 128]
            for piece in PAIR:
                sq_ref[which, :, piece] += part[piece * span:(piece + 1) * span].reshape(n_seq, PIECE, 128)

        @pl.when(step < n_tiles)
        def _():
            normed_out(wq_ref, q_ref, 0)

        @pl.when((step >= n_tiles) & (step < 2 * n_tiles))
        def _():
            normed_out(wk_ref, k_ref, 1)

        @pl.when(step >= 2 * n_tiles)
        def _():
            put(v_ref, dot(lhs[...], wv_ref[...]).astype(jnp.bfloat16))

    def phase(step, which):
        return jnp.clip(step - which * n_tiles, 0, n_tiles - 1)

    def w_spec(which):
        return pl.BlockSpec((d_model, TILE), lambda j, m: (0, core_tile(phase(j, which), m[1])))

    def o_spec(which):
        return pl.BlockSpec((n_seq, 2, PIECE, TILE), lambda j, m: (0, 0, 0, phase(j, which)))

    act = whole((n_seq, PIECE, d_model))
    sums = (2, n_seq, 2, PIECE, 128)
    grid_spec = scalar_grid(
        3 * n_tiles, in_specs=[act, act, w_spec(0), w_spec(1), w_spec(2)],
        out_specs=[o_spec(0), o_spec(1), o_spec(2), fixed(sums)],
        scratch=[pltpu.VMEM((2 * span, d_model), jnp.bfloat16)])
    shape = (n_seq, 2, PIECE, half)
    return pl.pallas_call(
        body, grid_spec=grid_spec, name="qkv",
        out_shape=[jax.ShapeDtypeStruct(shape, jnp.float32), jax.ShapeDtypeStruct(shape, jnp.float32),
                   jax.ShapeDtypeStruct(shape, jnp.bfloat16), jax.ShapeDtypeStruct(sums, jnp.float32)],
        compiler_params=params(), cost_estimate=cost(2 * 2 * span * d_model * 3 * half, 3 * d_model * half * 2 + 2 ** 24),
    )(meta, first, second, w_query, w_key, w_value)


def attn_grad(meta, first, second, w_out):
    d_model = w_out.shape[0]
    half = d_model // 2
    n_seq = first.shape[0]
    span = n_seq * PIECE

    def body(meta_ref, a_ref, b_ref, w_ref, o_ref, lhs):
        @pl.when(pl.program_id(0) == 0)
        def _():
            lhs[0:span, :] = a_ref[...].reshape(span, d_model)
            lhs[span:, :] = b_ref[...].reshape(span, d_model)

        acc = dot(lhs[...], w_ref[...], NT).astype(jnp.bfloat16)
        for piece in PAIR:
            o_ref[:, piece] = acc[piece * span:(piece + 1) * span].reshape(n_seq, PIECE, TILE)

    act = whole((n_seq, PIECE, d_model))
    grid_spec = scalar_grid(
        half // TILE, in_specs=[act, act, pl.BlockSpec((TILE, d_model), lambda j, m: (core_tile(j, m[1]), 0))],
        out_specs=columns((n_seq, 2, PIECE, TILE)),
        scratch=[pltpu.VMEM((2 * span, d_model), jnp.bfloat16)])
    return pl.pallas_call(
        body, grid_spec=grid_spec, name="attn_grad",
        out_shape=jax.ShapeDtypeStruct((n_seq, 2, PIECE, half), jnp.bfloat16),
        compiler_params=params(), cost_estimate=cost(2 * 2 * span * d_model * half, d_model * half * 2 + 2 ** 23),
    )(meta, first, second, w_out)


def attention(meta, q_own, q_far, k_own, k_far, v_own, v_far, do_own, do_far, sums, cos_t, sin_t, g_query, g_key, seq, carried):
    half = q_own.shape[-1]
    n_heads = half // HEAD_DIM
    seq_len = 4 * PIECE
    wide = HEADS_STEP * HEAD_DIM
    scale = HEAD_DIM ** -0.5
    exp_scale = scale * math.log2(math.e)
    n_carried = len(carried)

    def body(meta_ref, qo, qx, ko, kx, vo, vx, doo, dox, no, ns, fo, fs, cos_ref, sin_ref, gq_ref, gk_ref, *rest):
        rest = rest[n_carried:]
        a_ref, dq_ref, dk_ref, dv_ref, at_ref, stat_ref, inv_ref, gain_ref, qs, ks, vs, dos, v_t, k_t, do_t, q_t, outs, dqs, dks, dvs = rest
        device, core = meta_ref[0], meta_ref[1]

        @pl.when(pl.program_id(0) == 0)
        def _():
            stat_ref[...] = jnp.zeros_like(stat_ref)
            for which in PAIR:
                for r in PIECES:
                    own, other = ((no, ns), (fo, fs))[r // 2]
                    both = own[which, 0, r % 2] + other[which, 0, 1 - r % 2]
                    inv = lax.rsqrt(row_sum(both) / (2 * half) + NORM_EPS)
                    inv_ref[which, r] = spread(inv)

        gains = (gq_ref[...].astype(jnp.float32), gk_ref[...].astype(jnp.float32))
        heads = [slice(i * HEAD_DIM, (i + 1) * HEAD_DIM) for i in range(HEADS_STEP)]

        def place(r):
            return pl.ds(pl.multiple_of(jnp.bitwise_xor(device, r) * PIECE, PIECE), PIECE)

        def normed(r, which, lanes):
            src = ((qo, qx), (ko, kx))[which][r // 2]
            return src[0, r % 2, :, lanes] * inv_ref[which, r]

        for r in PIECES:
            rows = place(r)
            vs[rows, :] = (vo, vx)[r // 2][0, r % 2]
            dos[rows, :] = (doo, dox)[r // 2][0, r % 2]
            for lanes in heads:
                for which, dst in ((0, qs), (1, ks)):
                    val = normed(r, which, lanes) * gains[which][:, lanes]
                    rot = val * cos_ref[r] + turn(val) * sin_ref[r]
                    dst[rows, lanes] = rot.astype(jnp.bfloat16)
        for lanes in heads:
            v_t[lanes, :] = vs[:, lanes].T
            k_t[lanes, :] = ks[:, lanes].T
            do_t[lanes, :] = dos[:, lanes].T
            q_t[lanes, :] = qs[:, lanes].T

        key_idx = lax.broadcasted_iota(jnp.int32, (PIECE, PIECE), 0)
        query_idx = lax.broadcasted_iota(jnp.int32, (PIECE, PIECE), 1)
        allowed = key_idx <= query_idx

        def products(unit):
            lanes, qi = unit
            cols = slice(qi * PIECE, (qi + 1) * PIECE)
            keys = (qi + 1) * PIECE
            return dot(ks[0:keys, lanes], q_t[lanes, cols]), dot(vs[0:keys, lanes], do_t[lanes, cols])

        order = [(lanes, qi) for qi in (3, 2, 1, 0) for lanes in heads]
        ahead = products(order[0])
        for pos, (lanes, qi) in enumerate(order):
            scores, d_probs = ahead
            if pos + 1 < len(order):
                ahead = products(order[pos + 1])
            low = qi * PIECE
            high = low + PIECE
            diag = jnp.where(allowed, scores[low:high, :], NEG_BIG)
            parts = [scores[0:low, :], diag] if qi else [diag]
            d_parts = [d_probs[0:low, :], d_probs[low:high, :]] if qi else [d_probs]
            top = parts[0].max(axis=0, keepdims=True)
            for s in parts[1:]:
                top = jnp.maximum(top, s.max(axis=0, keepdims=True))
            probs = [jnp.exp2((s - top) * exp_scale) for s in parts]
            total = sum(col_sum(p) for p in probs)
            inv_total = 1.0 / total
            probs = [p * inv_total for p in probs]
            row_dot = sum(col_sum((p * d)) for p, d in zip(probs, d_parts))
            d_scores = [(p * (d - row_dot)).astype(jnp.bfloat16) for p, d in zip(probs, d_parts)]
            probs_bf = [p.astype(jnp.bfloat16) for p in probs]
            d_scores = jnp.concatenate(d_scores, axis=0) if qi else d_scores[0]
            probs_bf = jnp.concatenate(probs_bf, axis=0) if qi else probs_bf[0]
            out_t = dot(v_t[lanes, 0:high], probs_bf)
            dq_t = dot(k_t[lanes, 0:high], d_scores)
            outs[low:high, lanes] = out_t.T.astype(jnp.bfloat16)
            spot = jnp.bitwise_xor(jnp.bitwise_xor(device, core), qi)
            at_ref[lanes, pl.ds(pl.multiple_of(spot * PIECE, PIECE), PIECE)] = out_t.astype(jnp.bfloat16)
            dqs[low:high, lanes] = dq_t.T
            dv_term = dot(probs_bf, dos[low:high, lanes])
            dk_term = dot(d_scores, qs[low:high, lanes])
            if qi == 3:
                dvs[:, lanes] = dv_term
                dks[:, lanes] = dk_term
            else:
                dvs[0:high, lanes] += dv_term
                dks[0:high, lanes] += dk_term

        gain_sums = [[0.0] * HEADS_STEP, [0.0] * HEADS_STEP]
        for r in PIECES:
            rows = place(r)
            slot = jnp.bitwise_xor(core, r)
            a_ref[0, slot] = outs[rows, :]
            dv_ref[0, slot] = dvs[rows, :].astype(jnp.bfloat16)
            for i, lanes in enumerate(heads):
                for which, src, dst in ((0, dqs, dq_ref), (1, dks, dk_ref)):
                    grad_bf = (src[rows, lanes] * scale).astype(jnp.bfloat16)
                    dst[0, slot, :, lanes] = grad_bf
                    grad = grad_bf.astype(jnp.float32)
                    back = grad * cos_ref[r] - turn(grad) * sin_ref[r]
                    term = back * normed(r, which, lanes)
                    gain_sums[which][i] = gain_sums[which][i] + col_sum(term)
                    stat_ref[which, r] += term * gains[which][:, lanes]
        for i, lanes in enumerate(heads):
            gain_ref[0, 0, :, lanes] = gain_sums[0][i]
            gain_ref[0, 1, :, lanes] = gain_sums[1][i]

    per_block = 8 // HEADS_STEP

    def act(arr):
        pick = seq if arr.shape[0] > 1 else 0
        return pl.BlockSpec((1, 2, PIECE, wide), lambda j, m: (pick, 0, 0, j))

    acts = [q_own, q_far, k_own, k_far, v_own, v_far, do_own, do_far]
    lane_sums = once((2, 1, 2, PIECE, HEAD_DIM), lambda j, m: (0, seq, 0, 0, 0))
    table = whole((4, PIECE, HEAD_DIM))
    gain = pl.BlockSpec((1, wide), lambda j, m: (0, core_tile(j, m[1], per_block)))
    big = pl.BlockSpec((1, 4, PIECE, wide), lambda j, m: (seq, 0, 0, j))
    col_bf = pltpu.VMEM((seq_len, wide), jnp.bfloat16)
    row_bf = pltpu.VMEM((wide, seq_len), jnp.bfloat16)
    col_f = pltpu.VMEM((seq_len, wide), jnp.float32)
    n_steps = n_heads // HEADS_STEP
    stat_spec = fixed((2, 4, PIECE, HEAD_DIM))
    stat_shape = jax.ShapeDtypeStruct((2, 4, PIECE, HEAD_DIM), jnp.float32)
    grid_spec = scalar_grid(
        n_steps, in_specs=[act(arr) for arr in acts] + [lane_sums] * 4 + [table, table, gain, gain] + [pl.BlockSpec(memory_space=pl.ANY)] * n_carried,
        out_specs=[big] * 4 + [pl.BlockSpec((wide, seq_len), lambda j, m: (j, seq)),
                               stat_spec, stat_spec,
                               pl.BlockSpec((1, 2, 1, wide), lambda j, m: (j, 0, 0, 0))],
        scratch=[col_bf] * 4 + [row_bf] * 4 + [col_bf] + [col_f] * 3)
    full = jax.ShapeDtypeStruct((2, 4, PIECE, half), jnp.bfloat16)
    flops = 6 * 2 * HEAD_DIM * 10 * PIECE * PIECE * n_heads
    return pl.pallas_call(
        body, grid_spec=grid_spec, name="attention",
        out_shape=[full] * 4 + [jax.ShapeDtypeStruct((half, 2 * seq_len), jnp.bfloat16), stat_shape, stat_shape,
                                jax.ShapeDtypeStruct((n_steps, 2, 1, wide), jnp.float32)],
        input_output_aliases={17 + i: i for i in range(n_carried)},
        compiler_params=params(), cost_estimate=cost(2 * flops, 5 * 2 ** 23, 10 * PIECE * PIECE * n_heads),
    )(meta, *acts, *sums, cos_t, sin_t, g_query, g_key, *carried)


def finish_grads(meta, d_query, d_key, raws, stats, stats_sib, invs, cos_t, sin_t, g_query, g_key):
    half = d_query.shape[-1]
    wide = 256
    n_steps = half // wide

    def body(meta_ref, dq_ref, dk_ref, qn, qf, kn, kf, s0, s1, t0, t1, i0, i1, cos_ref, sin_ref, gq_ref, gk_ref, oq_ref, ok_ref, mean):
        core = meta_ref[1]

        @pl.when(pl.program_id(0) == 0)
        def _():
            for seq in PAIR:
                for which in PAIR:
                    for r in PIECES:
                        both = (s0, s1)[seq][which, r] + (t0, t1)[seq][which, r ^ 1]
                        row = row_sum(both) / (2 * half)
                        mean[seq, which, r] = spread(row)

        for which, (d_ref, near, far, g_ref, o_ref) in enumerate(((dq_ref, qn, qf, gq_ref, oq_ref), (dk_ref, kn, kf, gk_ref, ok_ref))):
            for seq in PAIR:
                for r in PIECES:
                    slot = jnp.bitwise_xor(core, r)
                    scl = (i0, i1)[seq][which, r]
                    for lane in range(0, wide, HEAD_DIM):
                        lanes = slice(lane, lane + HEAD_DIM)
                        grad = d_ref[seq, slot, :, lanes].astype(jnp.float32)
                        back = grad * cos_ref[seq, r] - turn(grad) * sin_ref[seq, r]
                        normed = (near, far)[r // 2][seq, r % 2, :, lanes] * scl
                        gain = g_ref[:, lanes].astype(jnp.float32)
                        o_ref[seq, slot, :, lanes] = (scl * (back * gain - normed * mean[seq, which, r])).astype(jnp.bfloat16)


    big = columns((2, 4, PIECE, wide))
    raw = columns((2, 2, PIECE, wide))
    table = whole((2, 4, PIECE, HEAD_DIM))
    gain = pl.BlockSpec((1, wide), lambda j, m: (0, core_tile(j, m[1], 4)))
    grid_spec = scalar_grid(
        n_steps, in_specs=[big, big] + [raw] * 4 + [table] * 8 + [gain, gain],
        out_specs=[big, big], scratch=[pltpu.VMEM((2, 2, 4, PIECE, HEAD_DIM), jnp.float32)])
    return pl.pallas_call(
        body, grid_spec=grid_spec, name="finish",
        out_shape=[jax.ShapeDtypeStruct(d_query.shape, jnp.bfloat16)] * 2,
        compiler_params=params(), cost_estimate=cost(20 * d_query.size, 16 * d_query.size),
    )(meta, d_query, d_key, *raws, *stats, *stats_sib, *invs, cos_t, sin_t, g_query, g_key)


def rows_transposed(meta, own, sib, far, far_sib):
    d_model = own.shape[-1]
    rows = d_model // 4

    def body(meta_ref, *refs):
        core = meta_ref[1]
        for seq in PAIR:
            for r in PIECES:
                spot = pl.multiple_of((seq * 4 + jnp.bitwise_xor(core, r)) * PIECE, PIECE)
                refs[4][:, pl.ds(spot, PIECE)] = refs[r][seq].T

    act = pl.BlockSpec((2, PIECE, rows), lambda j, m: (0, 0, m[0]))
    grid_spec = scalar_grid(
        1, in_specs=[act] * 4,
        out_specs=fixed((rows, 8 * PIECE)))
    return pl.pallas_call(
        body, grid_spec=grid_spec, name="rows_transposed",
        out_shape=jax.ShapeDtypeStruct((rows, 8 * PIECE), jnp.bfloat16),
        compiler_params=params(), cost_estimate=cost(8 * PIECE * rows, 4 * 8 * PIECE * rows),
    )(meta, own, sib, far, far_sib)


def out_project(meta, a_own, a_sib, w_out, x_loc):
    d_model = w_out.shape[0]
    half = d_model // 2
    quarter = half // 2

    def body(meta_ref, own_ref, sib_ref, w0, w1, w2, w3, x_ref, y_ref, lhs):
        @pl.when(pl.program_id(0) == 0)
        def _():
            for seq in PAIR:
                lhs[seq * PIECE:(seq + 1) * PIECE, 0:half] = own_ref[seq, 0]
                lhs[seq * PIECE:(seq + 1) * PIECE, half:] = sib_ref[seq]

        acc = dot(lhs[:, 0:quarter], w0[...])
        for i, w in enumerate((w1, w2, w3), 1):
            acc = acc + dot(lhs[:, i * quarter:(i + 1) * quarter], w[...])
        y_ref[...] = (x_ref[...].astype(jnp.float32) + acc.reshape(x_ref.shape)).astype(jnp.bfloat16)

    def w_spec(i):
        return pl.BlockSpec((quarter, TILE), lambda j, m: (half_block(i, m[1]), j))

    act = columns((2, PIECE, TILE))
    grid_spec = scalar_grid(
        d_model // TILE, in_specs=[once((2, 1, PIECE, half), lambda j, m: (0, m[1], 0, 0)), whole((2, PIECE, half))]
        + [w_spec(i) for i in range(4)] + [act],
        out_specs=act, scratch=[pltpu.VMEM((2 * PIECE, d_model), jnp.bfloat16)])
    return pl.pallas_call(
        body, grid_spec=grid_spec, name="out_project",
        out_shape=jax.ShapeDtypeStruct(x_loc.shape, jnp.bfloat16),
        compiler_params=params(), cost_estimate=cost(2 * 2 * PIECE * d_model * d_model, d_model * d_model * 2 + 2 ** 24),
    )(meta, a_own, a_sib, w_out, w_out, w_out, w_out, x_loc)


def hidden_grad(meta, owns, sibs, weights, x_loc, grad_y, g_norm):
    d_model = weights[0].shape[0]
    half = d_model // 2
    quarter = half // 2
    tile = TILE
    n_steps = d_model // tile
    chunk = 32

    def body(meta_ref, *refs):
        acts, ws = refs[:6], refs[6:18]
        x_any, gy_any, g_ref, o_ref, part_ref, grad, x_ref, gy_ref, sems = refs[18:]
        step = pl.program_id(0)
        copies = [pltpu.make_async_copy(x_any, x_ref, sems.at[0]), pltpu.make_async_copy(gy_any, gy_ref, sems.at[1])]

        @pl.when(step == 0)
        def _():
            for copy in copies:
                copy.start()

        acc = None
        for i in range(3):
            for part in PAIR:
                lhs = acts[2 * i + part][...].reshape(2 * PIECE, half)
                for blk in PAIR:
                    term = dot(lhs[:, blk * quarter:(blk + 1) * quarter], ws[4 * i + 2 * part + blk][...], NT)
                    acc = term if acc is None else acc + term
        grad[:, pl.ds(pl.multiple_of(step * tile, tile), tile)] = acc

        @pl.when(step == n_steps - 1)
        def _():
            for copy in copies:
                copy.wait()
            part_ref[...] = jnp.zeros_like(part_ref)
            gain = g_ref[...].astype(jnp.float32)

            @pl.loop(0, 2 * PIECE // chunk)
            def _(i):
                rows = pl.ds(pl.multiple_of(i * chunk, chunk), chunk)
                val = x_ref[rows, :].astype(jnp.float32)
                inv = lax.rsqrt(row_sum(val * val) / d_model + NORM_EPS)
                normed = val * inv
                d_out = grad[rows, :]
                part_ref[...] += col_sum(d_out * normed)
                d_normed = d_out * gain
                d_in = inv * (d_normed - normed * (row_sum(d_normed * normed) / d_model))
                o_ref[rows, :] = (gy_ref[rows, :].astype(jnp.float32) + d_in).astype(jnp.bfloat16)

    def w_spec(i):
        return pl.BlockSpec((tile, quarter), lambda j, m: (j, half_block(i, m[1])))

    own = once((2, 1, PIECE, half), lambda j, m: (0, m[1], 0, 0))
    flat = (2 * PIECE, d_model)
    vec = (1, d_model)
    grid_spec = scalar_grid(
        n_steps, in_specs=[own] * 6 + [w_spec(i) for i in range(4)] * 3 + [pl.BlockSpec(memory_space=pl.ANY)] * 2 + [whole(vec)],
        out_specs=[whole(flat), whole(vec)],
        scratch=[pltpu.VMEM(flat, jnp.float32), pltpu.VMEM(flat, jnp.bfloat16), pltpu.VMEM(flat, jnp.bfloat16), pltpu.SemaphoreType.DMA((2,))])
    acts = [a for pair in zip(owns, sibs) for a in pair]
    mats = [w for w in weights for _ in range(4)]
    return pl.pallas_call(
        body, grid_spec=grid_spec, name="hidden_grad",
        out_shape=[jax.ShapeDtypeStruct(flat, jnp.bfloat16), jax.ShapeDtypeStruct(vec, jnp.float32)],
        compiler_params=params(), cost_estimate=cost(6 * 2 * PIECE * d_model * d_model, 6 * d_model * d_model + 2 ** 24),
    )(meta, *acts, *mats, x_loc.reshape(flat), grad_y.reshape(flat), g_norm)


def weight_grads(meta, rows_t, owns, sibs):
    rows, tokens = rows_t.shape
    half = owns[0].shape[-1]
    n_tiles = half // TILE
    per = 2 * n_tiles
    n_mats = len(owns)

    def body(meta_ref, lhs_ref, *refs):
        step = pl.program_id(0)
        for i in range(2 * n_mats):
            @pl.when((step >= i * n_tiles) & (step < (i + 1) * n_tiles))
            def _(i=i):
                refs[2 * n_mats + i // 2][...] = dot(lhs_ref[...], refs[i][...])

    def in_spec(i):
        return pl.BlockSpec((tokens, TILE), lambda j, m: (0, jnp.clip(j - i * n_tiles, 0, n_tiles - 1)))

    def out_spec(i):
        def tile(j, m):
            t = jnp.clip(j - i * per, 0, per - 1)
            return 0, core_tile(t % n_tiles, jnp.bitwise_xor(m[1], t // n_tiles))
        return pl.BlockSpec((rows, TILE), tile)

    grid_spec = scalar_grid(
        per * n_mats, in_specs=[whole((rows, tokens))] + [in_spec(i) for i in range(2 * n_mats)],
        out_specs=[out_spec(i) for i in range(n_mats)])
    mats = [a.reshape(tokens, half) for pair in zip(owns, sibs) for a in pair]
    return pl.pallas_call(
        body, grid_spec=grid_spec, name="weight_grads",
        out_shape=[jax.ShapeDtypeStruct((rows, 2 * half), jnp.float32)] * n_mats,
        compiler_params=params(),
        cost_estimate=cost(n_mats * 2 * rows * tokens * 2 * half, n_mats * (rows * half * 8 + tokens * half * 4)),
    )(meta, rows_t, *mats)


def out_weight_grad(meta, a_t, pieces):
    tokens = a_t.shape[1]
    rows = a_t.shape[0] // 2
    d_model = pieces[0][0].shape[-1]

    def body(meta_ref, a_ref, *refs):
        core = meta_ref[1]
        acc = None
        for i in range(8):
            spot = pl.multiple_of((i // 4 * 4 + jnp.bitwise_xor(core, i % 4)) * PIECE, PIECE)
            term = dot(a_ref[:, pl.ds(spot, PIECE)], refs[i][0])
            acc = term if acc is None else acc + term
        refs[8][...] = acc

    def spec(seq):
        return pl.BlockSpec((1, PIECE, TILE), lambda j, m: (seq, 0, j))

    grid_spec = scalar_grid(
        d_model // TILE, in_specs=[once((rows, tokens), lambda j, m: (m[2], 0))] + [spec(seq) for _, seq in pieces],
        out_specs=columns((rows, TILE)))
    return pl.pallas_call(
        body, grid_spec=grid_spec, name="out_weight_grad",
        out_shape=jax.ShapeDtypeStruct((rows, d_model), jnp.float32),
        compiler_params=params(), cost_estimate=cost(2 * rows * tokens * d_model, rows * d_model * 4 + tokens * d_model * 2),
    )(meta, a_t, *[arr for arr, _ in pieces])


def after(value, *others):
    return lax.optimization_barrier((value,) + others)[0]


def solution(mesh):
    to_sibling = functools.partial(lax.ppermute, axis_name='sp', perm=SIBLING)
    to_far = functools.partial(lax.ppermute, axis_name='sp', perm=CROSS)

    def device_step(x_loc, grad_y, positions, g_norm, w_query, w_key, w_value, w_out, g_query, g_key):
        n_batch, loc_len, d_model = x_loc.shape
        device = lax.axis_index('sp')
        core = device % 2
        chip = device // 2
        meta = jnp.stack([device, core, chip]).astype(jnp.int32)
        gq = g_query.reshape(1, d_model)
        gk = g_key.reshape(1, d_model)

        pos_far = to_far(positions)
        pos_sib = to_sibling(positions)
        gn = g_norm.reshape(1, d_model)
        gy = grad_y
        gy_sib = to_sibling(gy)
        hidden = input_norm(x_loc, gn)
        hidden, pos_far = lax.optimization_barrier((hidden, pos_far))
        h_far = to_far(hidden)
        h_sib = to_sibling(hidden)
        d_near = attn_grad(meta, after(gy, hidden), gy_sib, w_out)
        gy_late = after(gy, h_sib)
        gy_far = [to_far(gy_late[0:1]), to_far(gy_late[1:2])]

        qn, kn, vn, sums_near = qkv_project(meta, hidden, after(h_sib, d_near), w_query, w_key, w_value)
        sums_near_sib = to_sibling(sums_near)
        pos_fs = to_sibling(after(pos_far, sums_near))
        h_far = after(h_far, sums_near)
        h_fs = to_sibling(h_far)

        pos_all = jnp.stack([positions, pos_sib, pos_far, pos_fs], axis=1)
        half_dim = HEAD_DIM // 2
        inv_freq = ROPE_BASE ** (-jnp.arange(half_dim, dtype=jnp.float32) * (2.0 / HEAD_DIM))
        angles = pos_all.astype(jnp.float32)[..., None] * inv_freq
        cos_h, sin_h = jnp.cos(angles), jnp.sin(angles)
        cos_t = jnp.concatenate([cos_h, cos_h], axis=-1)
        sin_t = jnp.concatenate([-sin_h, sin_h], axis=-1)

        qf, kf, vf, sums_far = qkv_project(meta, h_far, h_fs, w_query, w_key, w_value)
        sums_far_sib = to_sibling(sums_far)
        sums = (sums_near, sums_near_sib, sums_far, sums_far_sib)
        gy_far[0] = after(gy_far[0], sums_far)
        gy_fs = [to_sibling(gy_far[0])]
        rows_t = rows_transposed(meta, hidden, h_sib, after(h_far, sums_far), h_fs)
        d_far = [attn_grad(meta, gy_far[0], after(gy_fs[0], rows_t), w_out)]

        stats, invs, gains = [], [], 0.0
        carried = ()
        for seq in PAIR:
            if seq == 1:
                gy_far[1] = after(gy_far[1], stats[0])
                gy_fs.append(to_sibling(gy_far[1]))
                d_far.append(attn_grad(meta, gy_far[1], gy_fs[1], w_out))
            *carried, stat, inv, gain = attention(meta, qn, qf, kn, kf, vn, vf, d_near, d_far[seq], sums, cos_t[seq], sin_t[seq], gq, gk, seq, carried)
            stats.append(stat)
            invs.append(inv)
            gains = gains + gain
        attended, dq_rot, dk_rot, dv, a_t = carried
        stats_sib = [to_sibling(stat) for stat in stats]
        a_out = lax.dynamic_index_in_dim(attended, 1 - core, axis=1, keepdims=False)
        a_sib = to_sibling(after(a_out, *stats_sib))
        dv_sib = to_sibling(after(dv, *stats_sib))
        dq, dk = finish_grads(meta, dq_rot, dk_rot, (qn, qf, kn, kf), stats, stats_sib, invs, cos_t, sin_t, gq, gk)
        dq, dk, a_sib, dv_sib = lax.optimization_barrier((dq, dk, a_sib, dv_sib))
        dq_sib, dk_sib = to_sibling(dq), to_sibling(dk)

        gy_pieces = []
        for seq in PAIR:
            gy_pieces += [(gy, seq), (gy_sib, seq), (gy_far[seq], 0), (gy_fs[seq], 0)]
        grad_w_out = out_weight_grad(meta, after(a_t, dq), gy_pieces)
        a_sib, grad_w_out = lax.optimization_barrier((a_sib, grad_w_out))
        y_out = out_project(meta, attended, a_sib, w_out, x_loc)
        dq_sib, dk_sib, y_out = lax.optimization_barrier((dq_sib, dk_sib, y_out))

        grad_x, part = hidden_grad(meta, [dq, dk, dv], [dq_sib, dk_sib, dv_sib], [w_query, w_key, w_value], x_loc, gy, gn)
        grad_x = grad_x.reshape(x_loc.shape)
        part = part.reshape(2, 2, d_model // 4)
        part = lax.dynamic_index_in_dim(part, chip, 0, False) + to_far(lax.dynamic_index_in_dim(part, 1 - chip, 0, False))
        grad_g_norm = lax.dynamic_index_in_dim(part, core, 0, False) + to_sibling(lax.dynamic_index_in_dim(part, 1 - core, 0, False))

        grad_w_value, grad_w_query, grad_w_key = weight_grads(meta, after(rows_t, grad_x), [dv, dq, dk], [dv_sib, dq_sib, dk_sib])
        gains = gains.reshape(2, -1, 2, HEADS_STEP * HEAD_DIM)
        gains = lax.dynamic_index_in_dim(gains, chip, 0, False)
        grad_g_query = gains[:, 0].reshape(-1)
        grad_g_key = gains[:, 1].reshape(-1)
        return y_out, grad_x, grad_g_norm, grad_w_query, grad_w_key, grad_w_value, grad_w_out, grad_g_query, grad_g_key

    seq_spec = P('dp', 'sp', None)
    mat_rep = P(None, None)
    vec_rep = P(None)
    row_spec = P(('dp', 'sp'), None)
    vec_spec = P(('dp', 'sp'))
    return jax.shard_map(device_step, mesh=mesh, in_specs=(seq_spec, seq_spec, P('dp', 'sp'), vec_rep, mat_rep, mat_rep, mat_rep, mat_rep, vec_rep, vec_rep), out_specs=(seq_spec, seq_spec, vec_spec, row_spec, row_spec, row_spec, row_spec, vec_spec, vec_spec), check_vma=False)
```
